16 devices in a mesh: data: 16 (over z, y, x, core).
Axes of the slice: x: 2, y: 2, z: 2, core: 2. Of those that a mesh axis runs over, the one named last changes fastest.
Arguments:
- q_in: bfloat16 [1024, 1024], P('data')
- d_in: bfloat16 [2, 1024, 1024], P(None, 'data')
- temperature: float32 [], replicated
- q_w1: bfloat16 [2, 1024, 4096], replicated
- q_w2: bfloat16 [2, 4096, 1024], replicated
- q_proj: bfloat16 [1024, 1024], replicated
- d_w1: bfloat16 [2, 1024, 4096], replicated
- d_w2: bfloat16 [2, 4096, 1024], replicated
- d_proj: bfloat16 [1024, 1024], replicated
Outputs:
- output 1: float32 [], replicated
- output 2: float32 [2, 1024, 4096], replicated
- output 3: float32 [2, 4096, 1024], replicated
- output 4: float32 [1024, 1024], replicated
- output 5: float32 [2, 1024, 4096], replicated
- output 6: float32 [2, 4096, 1024], replicated
- output 7: float32 [1024, 1024], replicated
All inputs are finite; a program needn't handle non-finite values.
Results may differ from the reference program's by a relative error of at most 0.0113187.
Values are sent between devices in bfloat16 or wider.
A program may use at most 1 GiB of HBM per device.

```python
import math
import jax
import jax.numpy as jnp
from jax import lax

GLOBAL_BATCH = 1024
SHARD_ROWS = 64
HIDDEN = 1024
FFN_WIDTH = 4096
REPR_DIM = 1024


def setup_inputs(seed: int = 0) -> dict:
    key_list = jax.random.split(jax.random.key(seed), 9)
    sharpness = 0.8 * math.sqrt(2.0 * math.log(2.0 * GLOBAL_BATCH))
    tau_base = 2.0 * math.sqrt(REPR_DIM) / sharpness

    def weight(w_key, w_shape, fan_in):
        return (jax.random.normal(w_key, w_shape, jnp.float32) * fan_in ** -0.5).astype(jnp.bfloat16)

    return dict(
        q_in=jax.random.normal(key_list[0], (GLOBAL_BATCH, HIDDEN), jnp.float32).astype(jnp.bfloat16),
        d_in=jax.random.normal(key_list[1], (2, GLOBAL_BATCH, HIDDEN), jnp.float32).astype(jnp.bfloat16),
        temperature=tau_base * jax.random.uniform(key_list[2], (), jnp.float32, 0.8, 1.25),
        q_w1=weight(key_list[3], (2, HIDDEN, FFN_WIDTH), HIDDEN),
        q_w2=weight(key_list[4], (2, FFN_WIDTH, HIDDEN), FFN_WIDTH),
        q_proj=weight(key_list[5], (HIDDEN, REPR_DIM), HIDDEN),
        d_w1=weight(key_list[6], (2, HIDDEN, FFN_WIDTH), HIDDEN),
        d_w2=weight(key_list[7], (2, FFN_WIDTH, HIDDEN), FFN_WIDTH),
        d_proj=weight(key_list[8], (HIDDEN, REPR_DIM), HIDDEN),
    )


def tower_forward(row_block, w_one, w_two, w_proj):
    hidden = row_block
    saved = []
    for layer in range(2):
        pre_act = jnp.dot(hidden, w_one[layer], preferred_element_type=jnp.float32)
        act_bf = jax.nn.gelu(pre_act).astype(jnp.bfloat16)
        saved.append((hidden, pre_act, act_bf))
        hidden = (hidden.astype(jnp.float32) + jnp.dot(act_bf, w_two[layer], preferred_element_type=jnp.float32)).astype(jnp.bfloat16)
    out_reps = jnp.dot(hidden, w_proj, preferred_element_type=jnp.float32).astype(jnp.bfloat16)
    return out_reps, hidden, saved


def tower_backward(upstream, w_one, w_two, w_proj, hidden, saved):
    g_proj = jnp.dot(hidden.T, upstream, preferred_element_type=jnp.float32)
    resid_grad = jnp.dot(upstream, w_proj.T, preferred_element_type=jnp.float32)
    grads_one = [None, None]
    grads_two = [None, None]
    for layer in (1, 0):
        h_in, pre_act, act_bf = saved[layer]
        resid_bf = resid_grad.astype(jnp.bfloat16)
        grads_two[layer] = jnp.dot(act_bf.T, resid_bf, preferred_element_type=jnp.float32)
        act_grad = jnp.dot(resid_bf, w_two[layer].T, preferred_element_type=jnp.float32)
        gelu_back = jax.vjp(jax.nn.gelu, pre_act)[1]
        pre_grad = gelu_back(act_grad)[0].astype(jnp.bfloat16)
        grads_one[layer] = jnp.dot(h_in.T, pre_grad, preferred_element_type=jnp.float32)
        if layer == 1:
            resid_grad = resid_grad + jnp.dot(pre_grad, w_one[layer].T, preferred_element_type=jnp.float32)
    return jnp.stack(grads_one), jnp.stack(grads_two), g_proj


def tower_grads(row_blocks, up_blocks, w_one, w_two, w_proj):
    def body(running, block_in):
        row_block, upstream = block_in
        hidden, saved = tower_forward(row_block, w_one, w_two, w_proj)[1:]
        new_grads = tower_backward(upstream, w_one, w_two, w_proj, hidden, saved)
        return tuple(old_sum + new_part for old_sum, new_part in zip(running, new_grads)), None

    zeros_init = (jnp.zeros(w_one.shape, jnp.float32), jnp.zeros(w_two.shape, jnp.float32), jnp.zeros(w_proj.shape, jnp.float32))
    return lax.scan(body, zeros_init, (row_blocks, up_blocks))[0]


def reference(q_in, d_in, temperature, q_w1, q_w2, q_proj, d_w1, d_w2, d_proj):
    n_blocks = GLOBAL_BATCH // SHARD_ROWS
    q_blocks = q_in.reshape(n_blocks, SHARD_ROWS, HIDDEN)
    d_blocks = d_in.reshape(n_blocks, 2 * SHARD_ROWS, HIDDEN)
    q_reps = lax.map(lambda row_block: tower_forward(row_block, q_w1, q_w2, q_proj)[0], q_blocks)
    doc_flat = lax.map(lambda row_block: tower_forward(row_block, d_w1, d_w2, d_proj)[0], d_blocks).reshape(2 * GLOBAL_BATCH, REPR_DIM)
    col_index = jnp.arange(2 * GLOBAL_BATCH)

    def loss_block(running, block_in):
        loss_sum, doc_grad = running
        q_block, block_index = block_in
        logits = jnp.dot(q_block, doc_flat.T, preferred_element_type=jnp.float32) / temperature
        row_index = block_index * SHARD_ROWS + jnp.arange(SHARD_ROWS)
        target = col_index[None, :] == row_index[:, None]
        log_norm = jax.nn.logsumexp(logits, axis=1)
        pos_logit = jnp.sum(jnp.where(target, logits, 0.0), axis=1)
        soft_prob = jnp.exp(logits - log_norm[:, None])
        grad_logit = ((soft_prob - target.astype(jnp.float32)) / (GLOBAL_BATCH * temperature)).astype(jnp.bfloat16)
        q_up = jnp.dot(grad_logit, doc_flat, preferred_element_type=jnp.float32).astype(jnp.bfloat16)
        doc_grad = doc_grad + jnp.dot(grad_logit.T, q_block, preferred_element_type=jnp.float32)
        return (loss_sum + jnp.sum(log_norm - pos_logit), doc_grad), q_up

    zeros_init = (jnp.zeros((), jnp.float32), jnp.zeros((2 * GLOBAL_BATCH, REPR_DIM), jnp.float32))
    final_state, q_up_blocks = lax.scan(loss_block, zeros_init, (q_reps, jnp.arange(n_blocks)))
    loss_sum, doc_grad = final_state
    doc_up_blocks = doc_grad.astype(jnp.bfloat16).reshape(n_blocks, 2 * SHARD_ROWS, REPR_DIM)
    q_one, q_two, q_pgrad = tower_grads(q_blocks, q_up_blocks, q_w1, q_w2, q_proj)
    d_one, d_two, d_pgrad = tower_grads(d_blocks, doc_up_blocks, d_w1, d_w2, d_proj)
    return (loss_sum / GLOBAL_BATCH, q_one, q_two, q_pgrad, d_one, d_two, d_pgrad)
```

```python
import jax
import jax.numpy as jnp
from jax import lax
from jax.sharding import PartitionSpec as P

ROWS_CONTRACT = (((0,), (0,)), ((), ()))
LAST_CONTRACT = (((1,), (1,)), ((), ()))
F32 = jnp.float32
BF16 = jnp.bfloat16


def dot(a, b):
    return jnp.dot(a, b, preferred_element_type=F32)


def dot_nt(a, b):
    return lax.dot_general(a, b, LAST_CONTRACT, preferred_element_type=F32)


def dot_tn(a, b):
    return lax.dot_general(a, b, ROWS_CONTRACT, preferred_element_type=F32)


def ffn(h, w1, w2):
    u = jax.nn.gelu(dot(h, w1)).astype(BF16)
    return (h.astype(F32) + dot(u, w2)).astype(BF16)


def gather(x):
    return lax.all_gather(x, 'data', axis=0, tiled=True)


def hidden_grads(h, e_bf, w1, w2):
    pre = dot(h, w1)
    u = jax.nn.gelu(pre).astype(BF16)
    t = dot_nt(e_bf, w2)
    delta = jax.vjp(jax.nn.gelu, pre)[1](t)[0].astype(BF16)
    return u, delta


def layer_grads(h, e_bf, w1, w2):
    u, delta = hidden_grads(h, e_bf, w1, w2)
    return dot_tn(h, delta), dot_tn(u, e_bf)


def local_step(q_loc, d_loc, temperature, q_w1, q_w2, q_proj, d_w1, d_w2, d_proj):
    rows = q_loc.shape[0]
    me = lax.axis_index('data')
    d_rows = d_loc.reshape(2 * rows, d_loc.shape[2])
    d_h = [d_rows]
    q_h = [q_loc]
    for k in range(2):
        d_h.append(ffn(d_h[k], d_w1[k], d_w2[k]))
    for k in range(2):
        q_h.append(ffn(q_h[k], q_w1[k], q_w2[k]))
    d_all = [gather(h) for h in d_h]
    q_all = [gather(h) for h in q_h]
    docs = dot(d_all[2], d_proj).astype(BF16)
    queries = dot(q_all[2], q_proj).astype(BF16)
    batch = queries.shape[0]
    logits = dot_nt(queries, docs) / temperature
    row = jnp.arange(batch)
    target = jnp.arange(2 * batch)[None, :] == ((row // rows) * 2 * rows + row % rows)[:, None]
    log_norm = jax.nn.logsumexp(logits, axis=1)
    pos = jnp.sum(jnp.where(target, logits, 0.0), axis=1)
    loss = jnp.sum(log_norm - pos) / batch
    prob = jnp.exp(logits - log_norm[:, None])
    grad = ((prob - target.astype(F32)) / (batch * temperature)).astype(BF16)
    q_up = dot(grad, docs).astype(BF16)
    d_up = dot_tn(grad, queries).astype(BF16)

    def tower(h_own, h_all, up, w1, w2, proj):
        own_rows = h_own[0].shape[0]
        g_proj = dot_tn(h_all[2], up)
        e1 = dot_nt(up, proj)
        e1_bf = e1.astype(BF16)
        e1_own = lax.dynamic_slice_in_dim(e1, me * own_rows, own_rows, 0)
        delta_own = hidden_grads(h_own[1], e1_own.astype(BF16), w1[1], w2[1])[1]
        e0_own = (e1_own + dot_nt(delta_own, w1[1])).astype(BF16)
        e0_bf = gather(e0_own)
        one1, two1 = layer_grads(h_all[1], e1_bf, w1[1], w2[1])
        one0, two0 = layer_grads(h_all[0], e0_bf, w1[0], w2[0])
        return jnp.stack([one0, one1]), jnp.stack([two0, two1]), g_proj

    d_grads = tower(d_h, d_all, d_up, d_w1, d_w2, d_proj)
    q_grads = tower(q_h, q_all, q_up, q_w1, q_w2, q_proj)
    return (loss, *q_grads, *d_grads)


def solution(mesh):
    specs_in = (P('data', None), P(None, 'data', None), P(), P(), P(), P(), P(), P(), P())
    specs_out = (P(), P(), P(), P(), P(), P(), P())
    return jax.shard_map(local_step, mesh=mesh, in_specs=specs_in, out_specs=specs_out, check_vma=False)
```

```python
import functools

import jax
import jax.numpy as jnp
from jax import lax
from jax.experimental import pallas as pl
from jax.experimental.pallas import tpu as pltpu
from jax.sharding import PartitionSpec as P

ROWS_CONTRACT = (((0,), (0,)), ((), ()))
LAST_CONTRACT = (((1,), (1,)), ((), ()))
F32 = jnp.float32
BF16 = jnp.bfloat16
GELU_C = 0.7978845608028654
GELU_D = 0.044715
MIB = 1024 * 1024


def dot(a, b):
    return jnp.dot(a, b, preferred_element_type=F32)


def dot_nt(a, b):
    return lax.dot_general(a, b, LAST_CONTRACT, preferred_element_type=F32)


def dot_tn(a, b):
    return lax.dot_general(a, b, ROWS_CONTRACT, preferred_element_type=F32)


def gelu_cdf(a):
    sq = a * a
    return sq, 0.5 + 0.5 * jnp.tanh(a * (GELU_C + (GELU_C * GELU_D) * sq))


def gelu_and_back(a, t):
    sq, cdf = gelu_cdf(a)
    u = a * cdf
    slope = cdf + u * (1.0 - cdf) * (2.0 * GELU_C + (6.0 * GELU_C * GELU_D) * sq)
    return u.astype(BF16), (slope * t).astype(BF16)


def gather_kernel(x_ref, out_ref, send_sem, recv_sem, pair_send, pair_recv, own_sem, own_pair):
    parts, rows = 3, x_ref.shape[0] // 3
    me = lax.axis_index('data')

    def flip(device, bit):
        return device + bit * (1 - 2 * (lax.div(device, bit) % 2))

    def walk(device, mask, axes):
        for i in range(3):
            if mask & (1 << i):
                device = flip(device, axes[i])
        return device

    partner = flip(me, 1)
    barrier = pltpu.get_barrier_semaphore()
    for bit in (1, 2, 4, 8):
        pl.semaphore_signal(barrier, inc=1, device_id=(flip(me, bit),), device_id_type=pl.DeviceIdType.MESH)
    pl.semaphore_wait(barrier, 4)

    started = []

    def piece(shard, p):
        return out_ref.at[shard, pl.ds(p * rows, rows)]

    def send(p, mask, step, axes):
        shard = walk(me, mask, axes)
        source = x_ref.at[pl.ds(p * rows, rows)] if mask == 0 else piece(shard, p)
        seen = mask | (1 << step)
        copy = pltpu.make_async_remote_copy(
            src_ref=source, dst_ref=piece(shard, p), send_sem=send_sem.at[p, seen], recv_sem=recv_sem.at[p, seen],
            device_id=(flip(me, axes[step]),), device_id_type=pl.DeviceIdType.MESH)
        copy.start()
        started.append(copy)

    def relay(p, mask, axes):
        shard = walk(me, mask, axes)
        copy = pltpu.make_async_remote_copy(
            src_ref=piece(shard, p), dst_ref=piece(shard, p), send_sem=pair_send.at[p, mask], recv_sem=pair_recv.at[p, mask],
            device_id=(partner,), device_id_type=pl.DeviceIdType.MESH)
        copy.start()
        pairs.append(copy)

    pairs = []
    orders = [(2, 4, 8), (4, 8, 2), (8, 2, 4)]
    for step in range(3):
        for p in range(parts):
            send(p, 0, step, orders[p])
    own = pltpu.make_async_copy(x_ref, out_ref.at[me], own_sem)
    own.start()
    pair_own = pltpu.make_async_remote_copy(
        src_ref=x_ref, dst_ref=out_ref.at[me], send_sem=own_pair.at[0], recv_sem=own_pair.at[1],
        device_id=(partner,), device_id_type=pl.DeviceIdType.MESH)
    pair_own.start()

    def arrived(p, mask):
        pltpu.make_async_remote_copy(
            src_ref=piece(me, p), dst_ref=piece(walk(me, mask, orders[p]), p), send_sem=send_sem.at[p, mask],
            recv_sem=recv_sem.at[p, mask], device_id=(partner,), device_id_type=pl.DeviceIdType.MESH).wait_recv()

    for mask in (1, 2, 3, 4, 5, 6, 7):
        first = 1 if mask == 1 else 2 if mask < 4 else 3
        for p in range(parts):
            arrived(p, mask)
            for step in range(first, 3):
                send(p, mask, step, orders[p])
            relay(p, mask, orders[p])
    for copy in started:
        copy.wait_send()
    for copy in pairs:
        copy.wait()
    own.wait()
    pair_own.wait()


def gather_rows(x):
    return pl.pallas_call(
        gather_kernel,
        out_shape=jax.ShapeDtypeStruct((16, *x.shape), x.dtype),
        in_specs=[pl.BlockSpec(memory_space=pltpu.VMEM)],
        out_specs=pl.BlockSpec(memory_space=pl.ANY),
        scratch_shapes=[pltpu.SemaphoreType.DMA((3, 8))] * 4 + [pltpu.SemaphoreType.DMA, pltpu.SemaphoreType.DMA((2,))],
        compiler_params=pltpu.CompilerParams(collective_id=0, has_side_effects=True),
        name='gather_rows',
    )(x)


def layer_kernel(row_tile, h_ref, e_ref, w1_ref, w2_ref, *rest):
    one_ref, two_ref, u_ref, delta_ref = rest[-4:]
    n, r, width = h_ref.shape
    h = h_ref.reshape(n * r, width)
    e = e_ref.reshape(n * r, width)
    w1_t = w1_ref[0].T
    for i in range(n * r // row_tile):
        rows = pl.ds(i * row_tile, row_tile)
        pre = dot_nt(w1_t, h[rows, :])
        t = dot_nt(w2_ref[0], e[rows, :])
        u_ref[:, rows], delta_ref[:, rows] = gelu_and_back(pre, t)
    for c in range(4):
        cols = pl.ds(c * (width // 4), width // 4)
        two_ref[0, :, cols] = dot(u_ref[...], e[:, cols])
        one_ref[0, cols, :] = dot(delta_ref[...], h[:, cols]).T


def layer_grads(layer, h_all, h_place, e_all, e_place, rows, w1, w2, grads=None):
    _, width, ffn_width = w1.shape
    n = h_all.shape[0]
    block = 512
    row_tile = 512
    total = n * rows
    in_specs = [
        pl.BlockSpec((n, rows, width), lambda j: (0, h_place, 0)),
        pl.BlockSpec((n, rows, width), lambda j: (0, e_place, 0)),
        pl.BlockSpec((1, width, block), lambda j: (layer, 0, j)),
        pl.BlockSpec((1, block, width), lambda j: (layer, j, 0)),
    ]
    args = [h_all, e_all, w1, w2]
    aliases = {}
    if grads is not None:
        in_specs += [pl.BlockSpec(memory_space=pl.ANY)] * 2
        args += list(grads)
        aliases = {4: 0, 5: 1}
    return pl.pallas_call(
        functools.partial(layer_kernel, row_tile),
        grid=(ffn_width // block,),
        in_specs=in_specs,
        out_specs=[
            pl.BlockSpec((1, width, block), lambda j: (layer, 0, j)),
            pl.BlockSpec((1, block, width), lambda j: (layer, j, 0)),
        ],
        out_shape=[jax.ShapeDtypeStruct(w1.shape, F32), jax.ShapeDtypeStruct(w2.shape, F32)],
        scratch_shapes=[pltpu.VMEM((block, total), BF16)] * 2,
        input_output_aliases=aliases,
        compiler_params=pltpu.CompilerParams(vmem_limit_bytes=56 * MIB, dimension_semantics=('arbitrary',)),
        cost_estimate=pl.CostEstimate(flops=8 * total * width * ffn_width, bytes_accessed=60 * MIB, transcendentals=0),
        name='layer_grads',
    )(*args)


def ffn(h, w1, w2):
    pre = dot(h, w1)
    u = (pre * gelu_cdf(pre)[1]).astype(BF16)
    return (h.astype(F32) + dot(u, w2)).astype(BF16)


def gather(x):
    return lax.all_gather(x, 'data', axis=0)


def local_step(q_loc, d_loc, temperature, q_w1, q_w2, q_proj, d_w1, d_w2, d_proj):
    rows, width = q_loc.shape
    me = lax.axis_index('data')
    d_h = [d_loc.reshape(2 * rows, width)]
    q_h = [q_loc]
    for k in range(2):
        d_h.append(ffn(d_h[k], d_w1[k], d_w2[k]))
        q_h.append(ffn(q_h[k], q_w1[k], q_w2[k]))
    h0_all = gather(jnp.concatenate([d_h[0], q_h[0]], axis=0))
    h1_all = gather(jnp.concatenate([d_h[1], q_h[1]], axis=0))
    h2_all = gather_rows(jnp.concatenate([d_h[2], q_h[2]], axis=0))
    d_last = h2_all[:, :2 * rows].reshape(-1, width)
    q_last = h2_all[:, 2 * rows:].reshape(-1, width)
    docs = dot(d_last, d_proj).astype(BF16)
    queries = dot(q_last, q_proj).astype(BF16)
    batch = queries.shape[0]
    logits = dot_nt(queries, docs) / temperature
    row = jnp.arange(batch)
    target = jnp.arange(2 * batch)[None, :] == ((row // rows) * 2 * rows + row % rows)[:, None]
    log_norm = jax.nn.logsumexp(logits, axis=1)
    pos = jnp.sum(jnp.where(target, logits, 0.0), axis=1)
    loss = jnp.sum(log_norm - pos) / batch
    prob = jnp.exp(logits - log_norm[:, None])
    grad = ((prob - target.astype(F32)) / (batch * temperature)).astype(BF16)
    q_up = dot(grad, docs).astype(BF16)
    d_up = dot_tn(grad, queries).astype(BF16)

    def chain(h1_own, up, w1, w2, proj):
        own = h1_own.shape[0]
        e1_bf = dot_nt(up, proj).astype(BF16)
        e1_own = dot_nt(lax.dynamic_slice_in_dim(up, me * own, own, 0), proj)
        delta = gelu_and_back(dot(h1_own, w1[1]), dot_nt(e1_own.astype(BF16), w2[1]))[1]
        return e1_bf.reshape(16, own, width), (e1_own + dot_nt(delta, w1[1])).astype(BF16)

    d_e1, d_e0 = chain(d_h[1], d_up, d_w1, d_w2, d_proj)
    q_e1, q_e0 = chain(q_h[1], q_up, q_w1, q_w2, q_proj)
    e0_all = gather(jnp.concatenate([d_e0, q_e0], axis=0))
    d_p = dot_tn(d_last, d_up)
    q_p = dot_tn(q_last, q_up)
    d_g = layer_grads(1, h1_all, 0, d_e1, 0, 2 * rows, d_w1, d_w2)
    q_g = layer_grads(1, h1_all, 2, q_e1, 0, rows, q_w1, q_w2)
    d_g = layer_grads(0, h0_all, 0, e0_all, 0, 2 * rows, d_w1, d_w2, d_g)
    q_g = layer_grads(0, h0_all, 2, e0_all, 2, rows, q_w1, q_w2, q_g)
    return (loss, *q_g, q_p, *d_g, d_p)


def solution(mesh):
    specs_in = (P('data', None), P(None, 'data', None), P(), P(), P(), P(), P(), P(), P())
    specs_out = (P(), P(), P(), P(), P(), P(), P())
    return jax.shard_map(local_step, mesh=mesh, in_specs=specs_in, out_specs=specs_out, check_vma=False)
```

```python
import functools

import jax
import jax.numpy as jnp
from jax import lax
from jax.experimental import pallas as pl
from jax.experimental.pallas import tpu as pltpu
from jax.sharding import PartitionSpec as P

ROWS_CONTRACT = (((0,), (0,)), ((), ()))
LAST_CONTRACT = (((1,), (1,)), ((), ()))
F32 = jnp.float32
BF16 = jnp.bfloat16
GELU_C = 0.7978845608028654
GELU_D = 0.044715
MIB = 1024 * 1024


def dot(a, b):
    return jnp.dot(a, b, preferred_element_type=F32)


def dot_nt(a, b):
    return lax.dot_general(a, b, LAST_CONTRACT, preferred_element_type=F32)


def dot_tn(a, b):
    return lax.dot_general(a, b, ROWS_CONTRACT, preferred_element_type=F32)


def gelu_cdf(a):
    sq = a * a
    return sq, 0.5 + 0.5 * jnp.tanh(a * (GELU_C + (GELU_C * GELU_D) * sq))


def gelu_and_back(a, t):
    sq, cdf = gelu_cdf(a)
    u = a * cdf
    slope = cdf + u * (1.0 - cdf) * (2.0 * GELU_C + (6.0 * GELU_C * GELU_D) * sq)
    return u.astype(BF16), (slope * t).astype(BF16)


def gather_kernel(x_ref, d_ref, q_ref, send_sem, recv_sem, pair_send, pair_recv, own_sem, own_send, own_recv):
    parts, rows = 3, x_ref.shape[0] // 3
    me = lax.axis_index('data')

    def flip(device, bit):
        return device + bit * (1 - 2 * (lax.div(device, bit) % 2))

    def walk(device, mask, axes):
        for i in range(3):
            if mask & (1 << i):
                device = flip(device, axes[i])
        return device

    partner = flip(me, 1)
    barrier = pltpu.get_barrier_semaphore()
    for bit in (1, 2, 4, 8):
        pl.semaphore_signal(barrier, inc=1, device_id=(flip(me, bit),), device_id_type=pl.DeviceIdType.MESH)
    pl.semaphore_wait(barrier, 4)

    started = []

    def piece(shard, p):
        return q_ref.at[shard] if p == 2 else d_ref.at[shard, pl.ds(p * rows, rows)]

    def send(p, mask, step, axes):
        shard = walk(me, mask, axes)
        source = x_ref.at[pl.ds(p * rows, rows)] if mask == 0 else piece(shard, p)
        seen = mask | (1 << step)
        copy = pltpu.make_async_remote_copy(
            src_ref=source, dst_ref=piece(shard, p), send_sem=send_sem.at[p, seen], recv_sem=recv_sem.at[p, seen],
            device_id=(flip(me, axes[step]),), device_id_type=pl.DeviceIdType.MESH)
        copy.start()
        started.append(copy)

    def relay(p, mask, axes):
        shard = walk(me, mask, axes)
        copy = pltpu.make_async_remote_copy(
            src_ref=piece(shard, p), dst_ref=piece(shard, p), send_sem=pair_send.at[p, mask], recv_sem=pair_recv.at[p, mask],
            device_id=(partner,), device_id_type=pl.DeviceIdType.MESH)
        copy.start()
        pairs.append(copy)

    pairs = []
    orders = [(2, 4, 8), (4, 8, 2), (8, 2, 4)]
    for step in range(3):
        for p in range(parts):
            send(p, 0, step, orders[p])
    owns = []
    for p in range(parts):
        source = x_ref.at[pl.ds(p * rows, rows)]
        own = pltpu.make_async_copy(source, piece(me, p), own_sem.at[p])
        own.start()
        owns.append(own)
        copy = pltpu.make_async_remote_copy(
            src_ref=source, dst_ref=piece(me, p), send_sem=own_send.at[p], recv_sem=own_recv.at[p],
            device_id=(partner,), device_id_type=pl.DeviceIdType.MESH)
        copy.start()
        pairs.append(copy)

    def arrived(p, mask):
        pltpu.make_async_remote_copy(
            src_ref=piece(me, p), dst_ref=piece(walk(me, mask, orders[p]), p), send_sem=send_sem.at[p, mask],
            recv_sem=recv_sem.at[p, mask], device_id=(partner,), device_id_type=pl.DeviceIdType.MESH).wait_recv()

    for mask in (1, 2, 3, 4, 5, 6, 7):
        first = 1 if mask == 1 else 2 if mask < 4 else 3
        for p in range(parts):
            arrived(p, mask)
            for step in range(first, 3):
                send(p, mask, step, orders[p])
            relay(p, mask, orders[p])
    for copy in started:
        copy.wait_send()
    for copy in pairs:
        copy.wait()
    for copy in owns:
        copy.wait()


def gather_rows(x):
    rows = x.shape[0] // 3
    return pl.pallas_call(
        gather_kernel,
        out_shape=[jax.ShapeDtypeStruct((16, 2 * rows, x.shape[1]), x.dtype), jax.ShapeDtypeStruct((16, rows, x.shape[1]), x.dtype)],
        in_specs=[pl.BlockSpec(memory_space=pltpu.VMEM)],
        out_specs=[pl.BlockSpec(memory_space=pl.ANY)] * 2,
        scratch_shapes=[pltpu.SemaphoreType.DMA((3, 8))] * 4 + [pltpu.SemaphoreType.DMA((3,))] * 3,
        compiler_params=pltpu.CompilerParams(collective_id=0, has_side_effects=True),
        name='gather_rows',
    )(x)


def layer_kernel(row_tile, in_place, incoming, send, core_ref, h_ref, e_ref, w1_ref, w2_ref, *rest):
    u_ref, delta_ref = rest[-2:]
    rest = rest[2 if in_place else 0:-2]
    if incoming:
        y_refs, rest = rest[:2], rest[4:]
        for y_ref, t_ref in zip(y_refs, rest[-2:]):
            t_ref[...] = y_ref[...]
        rest = rest[:-2]
    one_ref, two_ref = rest[:2]
    n, r, width = h_ref.shape
    h = h_ref.reshape(n * r, width)
    e = e_ref.reshape(n * r, width)
    w1_t = w1_ref[0].T
    for i in range(n * r // row_tile):
        rows = pl.ds(i * row_tile, row_tile)
        pre = dot_nt(w1_t, h[rows, :])
        t = dot_nt(w2_ref[0], e[rows, :])
        u_ref[:, rows], delta_ref[:, rows] = gelu_and_back(pre, t)
    for c in range(4):
        cols = pl.ds(c * (width // 4), width // 4)
        two = dot(u_ref[...], e[:, cols])
        one = dot(delta_ref[...], h[:, cols]).T
        two_ref[0, :, cols] = two
        one_ref[0, cols, :] = one
        if send:
            rest[3][0, :, cols] = two
            rest[2][0, cols, :] = one


def layer_grads(core, layer, first, h_all, h_place, e_all, e_place, rows, w1, w2, grads=None, incoming=None):
    _, width, ffn_width = w1.shape
    n = h_all.shape[0]
    block, row_tile, steps = 512, 512, 4
    total = n * rows
    send = first is None
    resident = pl.Buffered(buffer_count=1)

    def mine(j, c):
        return c[0] * steps + j if send else first + j

    def other(j, c):
        return (1 - c[0]) * steps + j

    def wide(at, place):
        return pl.BlockSpec((1, width, block), lambda j, c: (at, 0, place(j, c)))

    def tall(at, place):
        return pl.BlockSpec((1, block, width), lambda j, c: (at, place(j, c), 0))

    in_specs = [
        pl.BlockSpec((n, rows, width), lambda j, c: (0, h_place, 0), pipeline_mode=resident),
        pl.BlockSpec((n, rows, width), lambda j, c: (0, e_place, 0), pipeline_mode=resident),
        wide(layer, mine), tall(layer, mine),
    ]
    args = [core, h_all, e_all, w1, w2]
    out_specs = [wide(layer, mine), tall(layer, mine)]
    out_shape = [jax.ShapeDtypeStruct(w1.shape, F32), jax.ShapeDtypeStruct(w2.shape, F32)]
    aliases = {}
    anywhere = [pl.BlockSpec(memory_space=pl.ANY)] * 2
    if grads is not None:
        aliases.update({len(args): 0, len(args) + 1: 1})
        in_specs += anywhere
        args += list(grads)
    if send:
        out_specs += [wide(0, lambda j, c: j), tall(0, lambda j, c: j)]
        out_shape += [jax.ShapeDtypeStruct((1, width, ffn_width // 2), F32), jax.ShapeDtypeStruct((1, ffn_width // 2, width), F32)]
    if incoming is not None:
        at, halves, targets = incoming
        in_specs += [wide(0, lambda j, c: j), tall(0, lambda j, c: j)] + anywhere
        aliases.update({len(args) + 2: len(out_shape), len(args) + 3: len(out_shape) + 1})
        args += [*halves, *targets]
        out_specs += [wide(at, other), tall(at, other)]
        out_shape += [jax.ShapeDtypeStruct(t.shape, F32) for t in targets]
    out = pl.pallas_call(
        functools.partial(layer_kernel, row_tile, grads is not None, incoming is not None, send),
        grid_spec=pltpu.PrefetchScalarGridSpec(
            num_scalar_prefetch=1, grid=(steps,), in_specs=in_specs, out_specs=out_specs,
            scratch_shapes=[pltpu.VMEM((block, total), BF16)] * 2),
        out_shape=out_shape,
        input_output_aliases=aliases,
        compiler_params=pltpu.CompilerParams(vmem_limit_bytes=58 * MIB, dimension_semantics=('arbitrary',)),
        cost_estimate=pl.CostEstimate(flops=8 * total * width * block * steps, bytes_accessed=40 * MIB, transcendentals=0),
        name='layer_grads',
    )(*args)
    return [out[i:i + 2] for i in range(0, len(out), 2)]


def ffn(h, w1, w2):
    pre = dot(h, w1)
    u = (pre * gelu_cdf(pre)[1]).astype(BF16)
    return (h.astype(F32) + dot(u, w2)).astype(BF16)


def gather(x):
    return lax.all_gather(x, 'data', axis=0)


def local_step(q_loc, d_loc, temperature, q_w1, q_w2, q_proj, d_w1, d_w2, d_proj):
    rows, width = q_loc.shape
    me = lax.axis_index('data')
    own0 = lax.optimization_barrier(jnp.concatenate([d_loc.reshape(2 * rows, width), q_loc], axis=0))
    h0_all = gather(own0)
    d_h = [own0[:2 * rows]]
    q_h = [own0[2 * rows:]]
    for k in range(2):
        d_h.append(ffn(d_h[k], d_w1[k], d_w2[k]))
        q_h.append(ffn(q_h[k], q_w1[k], q_w2[k]))
    h1_all = gather(jnp.concatenate([d_h[1], q_h[1]], axis=0))
    d_last, q_last = [h.reshape(-1, width) for h in gather_rows(jnp.concatenate([d_h[2], q_h[2]], axis=0))]
    docs = dot(d_last, d_proj).astype(BF16)
    queries = dot(q_last, q_proj).astype(BF16)
    batch = queries.shape[0]
    logits = dot_nt(queries, docs) / temperature
    row = jnp.arange(batch)
    target = jnp.arange(2 * batch)[None, :] == ((row // rows) * 2 * rows + row % rows)[:, None]
    log_norm = jax.nn.logsumexp(logits, axis=1)
    pos = jnp.sum(jnp.where(target, logits, 0.0), axis=1)
    loss = jnp.sum(log_norm - pos) / batch
    prob = jnp.exp(logits - log_norm[:, None])
    grad = ((prob - target.astype(F32)) / (batch * temperature)).astype(BF16)
    q_up = dot(grad, docs).astype(BF16)
    d_up = dot_tn(grad, queries).astype(BF16)

    def chain(h1_own, up, w1, w2, proj):
        own = h1_own.shape[0]
        e1_bf = dot_nt(up, proj).astype(BF16)
        e1_own = dot_nt(lax.dynamic_slice_in_dim(up, me * own, own, 0), proj)
        delta = gelu_and_back(dot(h1_own, w1[1]), dot_nt(e1_own.astype(BF16), w2[1]))[1]
        return e1_bf.reshape(16, own, width), (e1_own + dot_nt(delta, w1[1])).astype(BF16)

    d_e1, d_e0 = chain(d_h[1], d_up, d_w1, d_w2, d_proj)
    q_e1, q_e0 = chain(q_h[1], q_up, q_w1, q_w2, q_proj)
    e0_all = gather(jnp.concatenate([d_e0, q_e0], axis=0))
    d_p = dot_tn(d_last, d_up)
    q_p = dot_tn(q_last, q_up)
    core = (me % 2).reshape(1)

    def swap(halves):
        return [lax.ppermute(x, 'data', [(i, i ^ 1) for i in range(16)]) for x in halves]

    q_g, q1 = layer_grads(core, 1, None, h1_all, 2, q_e1, 0, rows, q_w1, q_w2)
    q1 = swap(q1)
    d_g, d1 = layer_grads(core, 1, None, h1_all, 0, d_e1, 0, 2 * rows, d_w1, d_w2)
    d1 = swap(d1)
    d_g, d0, q_g = layer_grads(core, 0, None, h0_all, 0, e0_all, 0, 2 * rows, d_w1, d_w2, d_g, (1, q1, q_g))
    d0 = swap(d0)
    q_g, d_g = layer_grads(core, 0, 0, h0_all, 2, e0_all, 2, rows, q_w1, q_w2, q_g, (1, d1, d_g))
    q_g, d_g = layer_grads(core, 0, 4, h0_all, 2, e0_all, 2, rows, q_w1, q_w2, q_g, (0, d0, d_g))
    return (loss, *q_g, q_p, *d_g, d_p)


def solution(mesh):
    specs_in = (P('data', None), P(None, 'data', None), P(), P(), P(), P(), P(), P(), P())
    specs_out = (P(), P(), P(), P(), P(), P(), P())
    return jax.shard_map(local_step, mesh=mesh, in_specs=specs_in, out_specs=specs_out, check_vma=False)
```

```python
import functools

import jax
import jax.numpy as jnp
from jax import lax
from jax.experimental import pallas as pl
from jax.experimental.pallas import tpu as pltpu
from jax.sharding import PartitionSpec as P

ROWS_CONTRACT = (((0,), (0,)), ((), ()))
LAST_CONTRACT = (((1,), (1,)), ((), ()))
F32 = jnp.float32
BF16 = jnp.bfloat16
GELU_C = 0.7978845608028654
GELU_D = 0.044715
MIB = 1024 * 1024


def dot(a, b):
    return jnp.dot(a, b, preferred_element_type=F32)


def dot_nt(a, b):
    return lax.dot_general(a, b, LAST_CONTRACT, preferred_element_type=F32)


def dot_tn(a, b):
    return lax.dot_general(a, b, ROWS_CONTRACT, preferred_element_type=F32)


def gelu_cdf(a):
    sq = a * a
    return sq, 0.5 + 0.5 * jnp.tanh(a * (GELU_C + (GELU_C * GELU_D) * sq))


def gelu_and_back(a, t):
    sq, cdf = gelu_cdf(a)
    u = a * cdf
    slope = cdf + u * (1.0 - cdf) * (2.0 * GELU_C + (6.0 * GELU_C * GELU_D) * sq)
    return u.astype(BF16), (slope * t).astype(BF16)


BLOCK = 1024
THIRDS = ((0, 384), (384, 384), (768, 256))
ORDERS = ((2, 4, 8), (4, 8, 2), (8, 2, 4))


def flip(device, bit):
    return device + bit * (1 - 2 * (lax.div(device, bit) % 2))


def forward_kernel(x_ref, dw1_ref, dw2_ref, qw1_ref, qw2_ref, h1_ref, d_all, q_all, acc_ref, h_ref, h2_ref,
                   send_sem, recv_sem, pair_send, pair_recv, own_sem, own_send, own_recv):
    s = pl.program_id(0)
    per = pl.num_programs(0) // 4
    me = lax.axis_index('data')
    partner = flip(me, 1)
    d_rows = d_all.shape[1]
    q_rows = q_all.shape[1]
    towers = ((pl.ds(0, d_rows), d_all), (pl.ds(d_rows, q_rows), q_all))

    def walk(p, mask):
        device = me
        for i in range(3):
            if mask & (1 << i):
                device = flip(device, ORDERS[p][i])
        return device

    def remote(source, target, send, recv, device):
        return pltpu.make_async_remote_copy(src_ref=source, dst_ref=target, send_sem=send, recv_sem=recv,
                                            device_id=(device,), device_id_type=pl.DeviceIdType.MESH)

    def hop(t, p, mask, step):
        rows, out = towers[t]
        cols = pl.ds(*THIRDS[p])
        shard = walk(p, mask)
        source = h2_ref.at[rows, cols] if mask == 0 else out.at[shard, :, cols]
        seen = mask | (1 << step)
        return remote(source, out.at[shard, :, cols], send_sem.at[t, p, seen], recv_sem.at[t, p, seen], flip(me, ORDERS[p][step]))

    def relay(t, p, mask):
        part = towers[t][1].at[walk(p, mask), :, pl.ds(*THIRDS[p])]
        return remote(part, part, pair_send.at[t, p, mask], pair_recv.at[t, p, mask], partner)

    def arrived(t, p, mask):
        part = towers[t][1].at[walk(p, mask), :, pl.ds(*THIRDS[p])]
        remote(part, part, send_sem.at[t, p, mask], recv_sem.at[t, p, mask], partner).wait_recv()

    def own_pair(t):
        rows, out = towers[t]
        return remote(h2_ref.at[rows], out.at[me], own_send.at[t], own_recv.at[t], partner)

    def own_copy(t):
        rows, out = towers[t]
        return pltpu.make_async_copy(h2_ref.at[rows], out.at[me], own_sem.at[t])

    def begin(t):
        for step in range(3):
            for p in range(3):
                hop(t, p, 0, step).start()
        own_copy(t).start()
        own_pair(t).start()

    def onward(t, masks):
        for mask in masks:
            for p in range(3):
                arrived(t, p, mask)
                for step in range(mask.bit_length(), 3):
                    hop(t, p, mask, step).start()
                relay(t, p, mask).start()

    def layers(first, rows, w1_ref, w2_ref):
        @pl.when(s == first)
        def _():
            h_ref[rows, :] = x_ref[rows, :]

        @pl.when((s - first) % per == 0)
        def _():
            acc_ref[rows, :] = h_ref[rows, :].astype(F32)

        pre = dot(h_ref[rows, :], w1_ref[0])
        acc_ref[rows, :] += dot((pre * gelu_cdf(pre)[1]).astype(BF16), w2_ref[0])

        @pl.when(s == first + per - 1)
        def _():
            h1 = acc_ref[rows, :].astype(BF16)
            h_ref[rows, :] = h1
            h1_ref[rows, :] = h1

        @pl.when(s == first + 2 * per - 1)
        def _():
            h2_ref[rows, :] = acc_ref[rows, :].astype(BF16)

    @pl.when(s == 0)
    def _():
        barrier = pltpu.get_barrier_semaphore()
        for bit in (1, 2, 4, 8):
            pl.semaphore_signal(barrier, inc=1, device_id=(flip(me, bit),), device_id_type=pl.DeviceIdType.MESH)
        pl.semaphore_wait(barrier, 4)

    @pl.when(s == 2 * per)
    def _():
        begin(0)

    @pl.when(s == 2 * per + per // 2)
    def _():
        onward(0, (1,))

    @pl.when(s == 3 * per)
    def _():
        onward(0, (2,))

    @pl.when(s == 3 * per + per // 4)
    def _():
        onward(0, (3,))

    @pl.when(s < 2 * per)
    def _():
        layers(0, towers[0][0], dw1_ref, dw2_ref)

    @pl.when((s >= 2 * per) & (s < 4 * per))
    def _():
        layers(2 * per, towers[1][0], qw1_ref, qw2_ref)

    @pl.when(s == 4 * per)
    def _():
        begin(1)
        onward(0, (4, 5, 6, 7))
        onward(1, (1, 2, 3, 4, 5, 6, 7))
        for t in range(2):
            for p in range(3):
                for mask in range(8):
                    for step in range(mask.bit_length(), 3):
                        hop(t, p, mask, step).wait_send()
                    if mask:
                        relay(t, p, mask).wait()
            own_copy(t).wait()
            own_pair(t).wait()


def forward(own0, d_w1, d_w2, q_w1, q_w2):
    rows, width = own0.shape
    per = d_w1.shape[2] // BLOCK

    def place(s):
        f = s // (2 * per)
        return f - f // 2, f // 2, (s // per) % 2, s % per

    def at_d(s):
        f, _, layer, j = place(s)
        f = s // (2 * per)
        f = f - f // 2
        return layer * (1 - f) + f, j * (1 - f) + (per - 1) * f

    def at_q(s):
        f, end, layer, j = place(s)
        live = f - end
        return layer * live + end, j * live + (per - 1) * end

    def wide(at):
        return pl.BlockSpec((1, width, BLOCK), lambda s: (at(s)[0], 0, at(s)[1]))

    def tall(at):
        return pl.BlockSpec((1, BLOCK, width), lambda s: (at(s)[0], at(s)[1], 0))

    third = rows // 3
    sems = pltpu.SemaphoreType.DMA
    return pl.pallas_call(
        forward_kernel,
        grid=(4 * per + 1,),
        in_specs=[pl.BlockSpec((rows, width), lambda s: (0, 0)), wide(at_d), tall(at_d), wide(at_q), tall(at_q)],
        out_specs=[pl.BlockSpec((rows, width), lambda s: (0, 0))] + [pl.BlockSpec(memory_space=pl.ANY)] * 2,
        out_shape=[jax.ShapeDtypeStruct((rows, width), BF16), jax.ShapeDtypeStruct((16, 2 * third, width), BF16),
                   jax.ShapeDtypeStruct((16, third, width), BF16)],
        scratch_shapes=[pltpu.VMEM((rows, width), F32), pltpu.VMEM((rows, width), BF16), pltpu.VMEM((rows, width), BF16),
                        sems((2, 3, 8)), sems((2, 3, 8)), sems((2, 3, 8)), sems((2, 3, 8)), sems((2,)), sems((2,)), sems((2,))],
        compiler_params=pltpu.CompilerParams(collective_id=0, has_side_effects=True, dimension_semantics=('arbitrary',)),
        cost_estimate=pl.CostEstimate(flops=8 * rows * width * d_w1.shape[2], bytes_accessed=72 * MIB, transcendentals=0),
        name='forward',
    )(own0, d_w1, d_w2, q_w1, q_w2)


def chain_kernel(h_ref, e_ref, dw1_ref, dw2_ref, qw1_ref, qw2_ref, out_ref, acc_ref):
    s = pl.program_id(0)
    per = pl.num_programs(0) // 2
    third = h_ref.shape[0] // 3

    def block(rows, w1_ref, w2_ref):
        pre = dot(h_ref[rows, :], w1_ref[0])
        t = dot_nt(e_ref[rows, :].astype(BF16), w2_ref[0])
        acc_ref[rows, :] += dot_nt(gelu_and_back(pre, t)[1], w1_ref[0])

    @pl.when(s == 0)
    def _():
        acc_ref[...] = e_ref[...]

    @pl.when(s < per)
    def _():
        block(pl.ds(0, 2 * third), dw1_ref, dw2_ref)

    @pl.when(s >= per)
    def _():
        block(pl.ds(2 * third, third), qw1_ref, qw2_ref)

    @pl.when(s == 2 * per - 1)
    def _():
        out_ref[...] = acc_ref[...].astype(BF16)


def chain(h1_own, e1_own, d_w1, d_w2, q_w1, q_w2):
    rows, width = h1_own.shape
    per = d_w1.shape[2] // BLOCK

    def at_d(s):
        return (s % per) * (1 - s // per) + (per - 1) * (s // per)

    def at_q(s):
        return (s % per) * (s // per)

    def wide(at):
        return pl.BlockSpec((1, width, BLOCK), lambda s: (1, 0, at(s)))

    def tall(at):
        return pl.BlockSpec((1, BLOCK, width), lambda s: (1, at(s), 0))

    whole = pl.BlockSpec((rows, width), lambda s: (0, 0))
    return pl.pallas_call(
        chain_kernel,
        grid=(2 * per,),
        in_specs=[whole, whole, wide(at_d), tall(at_d), wide(at_q), tall(at_q)],
        out_specs=whole,
        out_shape=jax.ShapeDtypeStruct((rows, width), BF16),
        scratch_shapes=[pltpu.VMEM((rows, width), F32)],
        compiler_params=pltpu.CompilerParams(dimension_semantics=('arbitrary',)),
        cost_estimate=pl.CostEstimate(flops=4 * rows * width * d_w1.shape[2], bytes_accessed=36 * MIB, transcendentals=0),
        name='chain',
    )(h1_own, e1_own, d_w1, d_w2, q_w1, q_w2)


def layer_kernel(row_tile, in_place, incoming, send, core_ref, h_ref, e_ref, w1_ref, w2_ref, *rest):
    u_ref, delta_ref = rest[-2:]
    rest = rest[2 if in_place else 0:-2]
    if incoming:
        y_refs, rest = rest[:2], rest[4:]
        for y_ref, t_ref in zip(y_refs, rest[-2:]):
            t_ref[...] = y_ref[...]
        rest = rest[:-2]
    one_ref, two_ref = rest[:2]
    n, r, width = h_ref.shape
    h = h_ref.reshape(n * r, width)
    e = e_ref.reshape(n * r, width)
    w1_t = w1_ref[0].T
    for i in range(n * r // row_tile):
        rows = pl.ds(i * row_tile, row_tile)
        pre = dot_nt(w1_t, h[rows, :])
        t = dot_nt(w2_ref[0], e[rows, :])
        u_ref[:, rows], delta_ref[:, rows] = gelu_and_back(pre, t)
    for c in range(4):
        cols = pl.ds(c * (width // 4), width // 4)
        two = dot(u_ref[...], e[:, cols])
        one = dot(delta_ref[...], h[:, cols]).T
        two_ref[0, :, cols] = two
        one_ref[0, cols, :] = one
        if send:
            rest[3][0, :, cols] = two
            rest[2][0, cols, :] = one


def layer_grads(core, layer, first, h_all, h_place, e_all, e_place, rows, w1, w2, grads=None, incoming=None):
    _, width, ffn_width = w1.shape
    n = h_all.shape[0]
    block, row_tile, steps = 512, 512, 4
    total = n * rows
    send = first is None
    resident = pl.Buffered(buffer_count=1)

    def mine(j, c):
        return c[0] * steps + j if send else first + j

    def other(j, c):
        return (1 - c[0]) * steps + j

    def wide(at, place):
        return pl.BlockSpec((1, width, block), lambda j, c: (at, 0, place(j, c)))

    def tall(at, place):
        return pl.BlockSpec((1, block, width), lambda j, c: (at, place(j, c), 0))

    in_specs = [
        pl.BlockSpec((n, rows, width), lambda j, c: (0, h_place, 0), pipeline_mode=resident),
        pl.BlockSpec((n, rows, width), lambda j, c: (0, e_place, 0), pipeline_mode=resident),
        wide(layer, mine), tall(layer, mine),
    ]
    args = [core, h_all, e_all, w1, w2]
    out_specs = [wide(layer, mine), tall(layer, mine)]
    out_shape = [jax.ShapeDtypeStruct(w1.shape, F32), jax.ShapeDtypeStruct(w2.shape, F32)]
    aliases = {}
    anywhere = [pl.BlockSpec(memory_space=pl.ANY)] * 2
    if grads is not None:
        aliases.update({len(args): 0, len(args) + 1: 1})
        in_specs += anywhere
        args += list(grads)
    if send:
        out_specs += [wide(0, lambda j, c: j), tall(0, lambda j, c: j)]
        out_shape += [jax.ShapeDtypeStruct((1, width, ffn_width // 2), F32), jax.ShapeDtypeStruct((1, ffn_width // 2, width), F32)]
    if incoming is not None:
        at, halves, targets = incoming
        in_specs += [wide(0, lambda j, c: j), tall(0, lambda j, c: j)] + anywhere
        aliases.update({len(args) + 2: len(out_shape), len(args) + 3: len(out_shape) + 1})
        args += [*halves, *targets]
        out_specs += [wide(at, other), tall(at, other)]
        out_shape += [jax.ShapeDtypeStruct(t.shape, F32) for t in targets]
    out = pl.pallas_call(
        functools.partial(layer_kernel, row_tile, grads is not None, incoming is not None, send),
        grid_spec=pltpu.PrefetchScalarGridSpec(
            num_scalar_prefetch=1, grid=(steps,), in_specs=in_specs, out_specs=out_specs,
            scratch_shapes=[pltpu.VMEM((block, total), BF16)] * 2),
        out_shape=out_shape,
        input_output_aliases=aliases,
        compiler_params=pltpu.CompilerParams(vmem_limit_bytes=58 * MIB, dimension_semantics=('arbitrary',)),
        cost_estimate=pl.CostEstimate(flops=8 * total * width * block * steps, bytes_accessed=40 * MIB, transcendentals=0),
        name='layer_grads',
    )(*args)
    return [out[i:i + 2] for i in range(0, len(out), 2)]


def gather(x):
    return lax.all_gather(x, 'data', axis=0)


def local_step(q_loc, d_loc, temperature, q_w1, q_w2, q_proj, d_w1, d_w2, d_proj):
    rows, width = q_loc.shape
    me = lax.axis_index('data')
    own0 = jnp.concatenate([d_loc.reshape(2 * rows, width), q_loc], axis=0)
    h1_own, d_last, q_last = forward(own0, d_w1, d_w2, q_w1, q_w2)
    d_last = d_last.reshape(-1, width)
    q_last = q_last.reshape(-1, width)
    h1_all = gather(h1_own)
    h0_all = gather(lax.optimization_barrier((own0, h1_own))[0])
    docs = dot(d_last, d_proj).astype(BF16)
    queries = dot(q_last, q_proj).astype(BF16)
    batch = queries.shape[0]
    logits = dot_nt(queries, docs) / temperature
    row = jnp.arange(batch)
    target = jnp.arange(2 * batch)[None, :] == ((row // rows) * 2 * rows + row % rows)[:, None]
    log_norm = jax.nn.logsumexp(logits, axis=1)
    pos = jnp.sum(jnp.where(target, logits, 0.0), axis=1)
    loss = jnp.sum(log_norm - pos) / batch
    prob = jnp.exp(logits - log_norm[:, None])
    grad = ((prob - target.astype(F32)) / (batch * temperature)).astype(BF16)
    q_up = dot(grad, docs).astype(BF16)
    d_up = dot_tn(grad, queries).astype(BF16)

    def start(up, proj):
        own = up.shape[0] // 16
        e1_own = dot_nt(lax.dynamic_slice_in_dim(up, me * own, own, 0), proj)
        return dot_nt(up, proj).astype(BF16).reshape(16, own, width), e1_own

    d_e1, d_e1_own = start(d_up, d_proj)
    q_e1, q_e1_own = start(q_up, q_proj)
    e1_own = jnp.concatenate([d_e1_own, q_e1_own], axis=0)
    e0_all = gather(chain(h1_own, e1_own, d_w1, d_w2, q_w1, q_w2))
    d_p = dot_tn(d_last, d_up)
    q_p = dot_tn(q_last, q_up)
    core = (me % 2).reshape(1)

    def swap(halves):
        return [lax.ppermute(x, 'data', [(i, i ^ 1) for i in range(16)]) for x in halves]

    q_g, q1 = layer_grads(core, 1, None, h1_all, 2, q_e1, 0, rows, q_w1, q_w2)
    q1 = swap(q1)
    d_g, d1 = layer_grads(core, 1, None, h1_all, 0, d_e1, 0, 2 * rows, d_w1, d_w2)
    d1 = swap(d1)
    d_g, d0, q_g = layer_grads(core, 0, None, h0_all, 0, e0_all, 0, 2 * rows, d_w1, d_w2, d_g, (1, q1, q_g))
    d0 = swap(d0)
    q_g, d_g = layer_grads(core, 0, 0, h0_all, 2, e0_all, 2, rows, q_w1, q_w2, q_g, (1, d1, d_g))
    q_g, d_g = layer_grads(core, 0, 4, h0_all, 2, e0_all, 2, rows, q_w1, q_w2, q_g, (0, d0, d_g))
    return (loss, *q_g, q_p, *d_g, d_p)


def solution(mesh):
    specs_in = (P('data', None), P(None, 'data', None), P(), P(), P(), P(), P(), P(), P())
    specs_out = (P(), P(), P(), P(), P(), P(), P())
    return jax.shard_map(local_step, mesh=mesh, in_specs=specs_in, out_specs=specs_out, check_vma=False)
```

```python
import functools

import jax
import jax.numpy as jnp
from jax import lax
from jax.experimental import pallas as pl
from jax.experimental.pallas import tpu as pltpu
from jax.sharding import PartitionSpec as P

ROWS_CONTRACT = (((0,), (0,)), ((), ()))
LAST_CONTRACT = (((1,), (1,)), ((), ()))
F32 = jnp.float32
BF16 = jnp.bfloat16
GELU_C = 0.7978845608028654
GELU_D = 0.044715
MIB = 1024 * 1024


def dot(a, b):
    return jnp.dot(a, b, preferred_element_type=F32)


def dot_nt(a, b):
    return lax.dot_general(a, b, LAST_CONTRACT, preferred_element_type=F32)


def dot_tn(a, b):
    return lax.dot_general(a, b, ROWS_CONTRACT, preferred_element_type=F32)


def gelu_cdf(a):
    sq = a * a
    return sq, 0.5 + 0.5 * jnp.tanh(a * (GELU_C + (GELU_C * GELU_D) * sq))


def gelu_and_back(a, t):
    sq, cdf = gelu_cdf(a)
    u = a * cdf
    slope = cdf + u * (1.0 - cdf) * (2.0 * GELU_C + (6.0 * GELU_C * GELU_D) * sq)
    return u.astype(BF16), (slope * t).astype(BF16)


BLOCK = 1024
RING = 4
THIRDS = ((0, 384), (384, 384), (768, 256))
ORDERS = ((2, 4, 8), (4, 8, 2), (8, 2, 4))


def flip(device, bit):
    return device + bit * (1 - 2 * (lax.div(device, bit) % 2))


def forward_kernel(xd_ref, xq_ref, dw1_ref, dw2_ref, qw1_ref, qw2_ref, h1_ref, d_all, q_all, acc_ref, h_ref, h2_ref,
                   w1_buf, w2_buf, w1_sem, w2_sem, send_sem, recv_sem, pair_send, pair_recv, own_sem, own_send, own_recv):
    s = pl.program_id(0)
    per = dw1_ref.shape[2] // BLOCK
    slot = s % RING
    me = lax.axis_index('data')
    partner = flip(me, 1)
    d_rows = d_all.shape[1]
    q_rows = q_all.shape[1]
    towers = ((pl.ds(0, d_rows), d_all), (pl.ds(d_rows, q_rows), q_all))

    def walk(p, mask):
        device = me
        for i in range(3):
            if mask & (1 << i):
                device = flip(device, ORDERS[p][i])
        return device

    def remote(source, target, send, recv, device):
        return pltpu.make_async_remote_copy(src_ref=source, dst_ref=target, send_sem=send, recv_sem=recv,
                                            device_id=(device,), device_id_type=pl.DeviceIdType.MESH)

    def hop(t, p, mask, step):
        rows, out = towers[t]
        cols = pl.ds(*THIRDS[p])
        shard = walk(p, mask)
        source = h2_ref.at[rows, cols] if mask == 0 else out.at[shard, :, cols]
        seen = mask | (1 << step)
        return remote(source, out.at[shard, :, cols], send_sem.at[t, p, seen], recv_sem.at[t, p, seen], flip(me, ORDERS[p][step]))

    def relay(t, p, mask):
        part = towers[t][1].at[walk(p, mask), :, pl.ds(*THIRDS[p])]
        return remote(part, part, pair_send.at[t, p, mask], pair_recv.at[t, p, mask], partner)

    def arrived(t, p, mask):
        part = towers[t][1].at[walk(p, mask), :, pl.ds(*THIRDS[p])]
        remote(part, part, send_sem.at[t, p, mask], recv_sem.at[t, p, mask], partner).wait_recv()

    def own_pair(t):
        rows, out = towers[t]
        return remote(h2_ref.at[rows], out.at[me], own_send.at[t], own_recv.at[t], partner)

    def own_copy(t):
        rows, out = towers[t]
        return pltpu.make_async_copy(h2_ref.at[rows], out.at[me], own_sem.at[t])

    def begin(t):
        for step in range(3):
            for p in range(3):
                hop(t, p, 0, step).start()
        own_copy(t).start()
        own_pair(t).start()

    def onward(t, masks):
        for mask in masks:
            for p in range(3):
                arrived(t, p, mask)
                for step in range(mask.bit_length(), 3):
                    hop(t, p, mask, step).start()
                relay(t, p, mask).start()

    def blocks(step, w1_ref, w2_ref):
        layer = (step // per) % 2
        cols = pl.ds((step % per) * BLOCK, BLOCK)
        at = step % RING
        return (pltpu.make_async_copy(w1_ref.at[layer, :, cols], w1_buf.at[at], w1_sem.at[at]),
                pltpu.make_async_copy(w2_ref.at[layer, cols, :], w2_buf.at[at], w2_sem.at[at]))

    def fetch(step):
        @pl.when(step < 2 * per)
        def _():
            for copy in blocks(step, dw1_ref, dw2_ref):
                copy.start()

        @pl.when((step >= 2 * per) & (step < 4 * per))
        def _():
            for copy in blocks(step, qw1_ref, qw2_ref):
                copy.start()

    def layers(first, rows, x_ref, w1_ref, w2_ref):
        for copy in blocks(s, w1_ref, w2_ref):
            copy.wait()

        @pl.when(s == first)
        def _():
            h_ref[rows, :] = x_ref[...]

        @pl.when((s - first) % per == 0)
        def _():
            acc_ref[rows, :] = h_ref[rows, :].astype(F32)

        pre = dot(h_ref[rows, :], w1_buf[slot])
        acc_ref[rows, :] += dot((pre * gelu_cdf(pre)[1]).astype(BF16), w2_buf[slot])

        @pl.when(s == first + per - 1)
        def _():
            h1 = acc_ref[rows, :].astype(BF16)
            h_ref[rows, :] = h1
            h1_ref[rows, :] = h1

        @pl.when(s == first + 2 * per - 1)
        def _():
            h2_ref[rows, :] = acc_ref[rows, :].astype(BF16)

    @pl.when(s == 0)
    def _():
        for step in range(RING - 1):
            for copy in blocks(step, dw1_ref, dw2_ref):
                copy.start()
        barrier = pltpu.get_barrier_semaphore()
        for bit in (1, 2, 4, 8):
            pl.semaphore_signal(barrier, inc=1, device_id=(flip(me, bit),), device_id_type=pl.DeviceIdType.MESH)
        pl.semaphore_wait(barrier, 4)

    fetch(s + RING - 1)

    @pl.when(s == 2 * per)
    def _():
        begin(0)

    @pl.when(s == 2 * per + per // 2)
    def _():
        onward(0, (1,))

    @pl.when(s == 3 * per)
    def _():
        onward(0, (2,))

    @pl.when(s == 3 * per + per // 4)
    def _():
        onward(0, (3,))

    @pl.when(s < 2 * per)
    def _():
        layers(0, towers[0][0], xd_ref, dw1_ref, dw2_ref)

    @pl.when((s >= 2 * per) & (s < 4 * per))
    def _():
        layers(2 * per, towers[1][0], xq_ref, qw1_ref, qw2_ref)

    @pl.when(s == 4 * per)
    def _():
        begin(1)
        onward(0, (4, 5, 6, 7))
        onward(1, (1, 2, 3, 4, 5, 6, 7))
        for t in range(2):
            for p in range(3):
                for mask in range(8):
                    for step in range(mask.bit_length(), 3):
                        hop(t, p, mask, step).wait_send()
                    if mask:
                        relay(t, p, mask).wait()
            own_copy(t).wait()
            own_pair(t).wait()


def forward(d_own, q_own, d_w1, d_w2, q_w1, q_w2):
    third, width = q_own.shape
    rows = 3 * third
    per = d_w1.shape[2] // BLOCK

    anywhere = pl.BlockSpec(memory_space=pl.ANY)
    sems = pltpu.SemaphoreType.DMA
    return pl.pallas_call(
        forward_kernel,
        grid=(4 * per + 1,),
        in_specs=[pl.BlockSpec((2 * third, width), lambda s: (0, 0)), pl.BlockSpec((third, width), lambda s: (0, 0)),
                  *[anywhere] * 4],
        out_specs=[pl.BlockSpec((rows, width), lambda s: (0, 0))] + [anywhere] * 2,
        out_shape=[jax.ShapeDtypeStruct((rows, width), BF16), jax.ShapeDtypeStruct((16, 2 * third, width), BF16),
                   jax.ShapeDtypeStruct((16, third, width), BF16)],
        scratch_shapes=[pltpu.VMEM((rows, width), F32), pltpu.VMEM((rows, width), BF16), pltpu.VMEM((rows, width), BF16),
                        pltpu.VMEM((RING, width, BLOCK), BF16), pltpu.VMEM((RING, BLOCK, width), BF16), sems((RING,)), sems((RING,)),
                        sems((2, 3, 8)), sems((2, 3, 8)), sems((2, 3, 8)), sems((2, 3, 8)), sems((2,)), sems((2,)), sems((2,))],
        compiler_params=pltpu.CompilerParams(collective_id=0, has_side_effects=True, dimension_semantics=('arbitrary',)),
        cost_estimate=pl.CostEstimate(flops=8 * rows * width * d_w1.shape[2], bytes_accessed=72 * MIB, transcendentals=0),
        name='forward',
    )(d_own, q_own, d_w1, d_w2, q_w1, q_w2)


def chain_kernel(h_ref, de_ref, qe_ref, dw1_ref, dw2_ref, qw1_ref, qw2_ref, out_ref, acc_ref):
    s = pl.program_id(0)
    third = h_ref.shape[0] // 3
    parts = ((pl.ds(0, 2 * third), de_ref, dw1_ref, dw2_ref), (pl.ds(2 * third, third), qe_ref, qw1_ref, qw2_ref))

    @pl.when(s == 0)
    def _():
        for rows, e_ref, _, _ in parts:
            acc_ref[rows, :] = e_ref[...]

    pre = [dot(h_ref[rows, :], w1_ref[0]) for rows, _, w1_ref, _ in parts]
    t = [dot_nt(e_ref[...].astype(BF16), w2_ref[0]) for _, e_ref, _, w2_ref in parts]
    delta = [gelu_and_back(*pair)[1] for pair in zip(pre, t)]
    for (rows, _, w1_ref, _), d in zip(parts, delta):
        acc_ref[rows, :] += dot_nt(d, w1_ref[0])

    @pl.when(s == pl.num_programs(0) - 1)
    def _():
        out_ref[...] = acc_ref[...].astype(BF16)


def chain(h1_own, d_e1, q_e1, d_w1, d_w2, q_w1, q_w2):
    rows, width = h1_own.shape
    block = 512
    wide = pl.BlockSpec((1, width, block), lambda s: (1, 0, s))
    tall = pl.BlockSpec((1, block, width), lambda s: (1, s, 0))

    def whole(x):
        return pl.BlockSpec(x.shape, lambda s: (0, 0))

    return pl.pallas_call(
        chain_kernel,
        grid=(d_w1.shape[2] // block,),
        in_specs=[whole(h1_own), whole(d_e1), whole(q_e1), wide, tall, wide, tall],
        out_specs=whole(h1_own),
        out_shape=jax.ShapeDtypeStruct((rows, width), BF16),
        scratch_shapes=[pltpu.VMEM((rows, width), F32)],
        compiler_params=pltpu.CompilerParams(dimension_semantics=('arbitrary',)),
        cost_estimate=pl.CostEstimate(flops=4 * rows * width * d_w1.shape[2], bytes_accessed=36 * MIB, transcendentals=0),
        name='chain',
    )(h1_own, d_e1, q_e1, d_w1, d_w2, q_w1, q_w2)


def layer_kernel(row_tile, in_place, incoming, send, top, core_ref, h_ref, e_ref, w1_ref, w2_ref, *rest):
    if top:
        up_ref, (proj_ref, last_ref), e_ref, rest = e_ref, rest[:2], rest[-1], rest[2:-1]
    u_ref, delta_ref = rest[-2:]
    rest = rest[2 if in_place else 0:-2]
    if incoming:
        y_refs, rest = rest[:2], rest[4:]
        for y_ref, t_ref in zip(y_refs, rest[-2:]):
            t_ref[...] = y_ref[...]
        rest = rest[:-2]
    one_ref, two_ref = rest[:2]
    n, r, width = h_ref.shape
    h = h_ref.reshape(n * r, width)
    e = e_ref.reshape(n * r, width)
    if top:
        up = up_ref.reshape(n * r, width)

        @pl.when(pl.program_id(0) == 0)
        def _():
            for i in range(n * r // row_tile):
                rows = pl.ds(i * row_tile, row_tile)
                e_ref[rows, :] = dot_nt(up[rows, :], proj_ref[...]).astype(BF16)

        rest[4][...] = dot_tn(last_ref.reshape(n * r, last_ref.shape[2])[...], up[...])
    w1_t = w1_ref[0].T
    for i in range(n * r // row_tile):
        rows = pl.ds(i * row_tile, row_tile)
        pre = dot_nt(w1_t, h[rows, :])
        t = dot_nt(w2_ref[0], e[rows, :])
        u_ref[:, rows], delta_ref[:, rows] = gelu_and_back(pre, t)
    for c in range(4):
        cols = pl.ds(c * (width // 4), width // 4)
        two = dot(u_ref[...], e[:, cols])
        one = dot(delta_ref[...], h[:, cols]).T
        two_ref[0, :, cols] = two
        one_ref[0, cols, :] = one
        if send:
            rest[3][0, :, cols] = two
            rest[2][0, cols, :] = one


def layer_grads(core, layer, first, h_all, h_place, e_all, e_place, rows, w1, w2, grads=None, incoming=None, top=None):
    _, width, ffn_width = w1.shape
    n = h_all.shape[0]
    block, row_tile, steps = 512, 512, 4
    total = n * rows
    send = first is None
    resident = pl.Buffered(buffer_count=1)

    def mine(j, c):
        return c[0] * steps + j if send else first + j

    def other(j, c):
        return (1 - c[0]) * steps + j

    def wide(at, place):
        return pl.BlockSpec((1, width, block), lambda j, c: (at, 0, place(j, c)))

    def tall(at, place):
        return pl.BlockSpec((1, block, width), lambda j, c: (at, place(j, c), 0))

    in_specs = [
        pl.BlockSpec((n, rows, width), lambda j, c: (0, h_place, 0), pipeline_mode=resident),
        pl.BlockSpec((n, rows, width), lambda j, c: (0, e_place, 0), pipeline_mode=resident),
        wide(layer, mine), tall(layer, mine),
    ]
    args = [core, h_all, e_all, w1, w2]
    out_specs = [wide(layer, mine), tall(layer, mine)]
    out_shape = [jax.ShapeDtypeStruct(w1.shape, F32), jax.ShapeDtypeStruct(w2.shape, F32)]
    aliases = {}
    anywhere = [pl.BlockSpec(memory_space=pl.ANY)] * 2
    scratch = [pltpu.VMEM((block, total), BF16)] * 2
    if top is not None:
        in_specs += [pl.BlockSpec((width, width), lambda j, c: (0, 0), pipeline_mode=resident),
                     pl.BlockSpec((n, rows, width // steps), lambda j, c: (0, 0, j))]
        args += list(top)
        scratch.append(pltpu.VMEM((total, width), BF16))
    if grads is not None:
        aliases.update({len(args): 0, len(args) + 1: 1})
        in_specs += anywhere
        args += list(grads)
    if send:
        out_specs += [wide(0, lambda j, c: j), tall(0, lambda j, c: j)]
        out_shape += [jax.ShapeDtypeStruct((1, width, ffn_width // 2), F32), jax.ShapeDtypeStruct((1, ffn_width // 2, width), F32)]
    if top is not None:
        out_specs.append(pl.BlockSpec((width // steps, width), lambda j, c: (j, 0)))
        out_shape.append(jax.ShapeDtypeStruct((width, width), F32))
    if incoming is not None:
        at, halves, targets = incoming
        in_specs += [wide(0, lambda j, c: j), tall(0, lambda j, c: j)] + anywhere
        aliases.update({len(args) + 2: len(out_shape), len(args) + 3: len(out_shape) + 1})
        args += [*halves, *targets]
        out_specs += [wide(at, other), tall(at, other)]
        out_shape += [jax.ShapeDtypeStruct(t.shape, F32) for t in targets]
    out = pl.pallas_call(
        functools.partial(layer_kernel, row_tile, grads is not None, incoming is not None, send, top is not None),
        grid_spec=pltpu.PrefetchScalarGridSpec(
            num_scalar_prefetch=1, grid=(steps,), in_specs=in_specs, out_specs=out_specs,
            scratch_shapes=scratch),
        out_shape=out_shape,
        input_output_aliases=aliases,
        compiler_params=pltpu.CompilerParams(vmem_limit_bytes=58 * MIB, dimension_semantics=('arbitrary',)),
        cost_estimate=pl.CostEstimate(flops=8 * total * width * block * steps, bytes_accessed=40 * MIB, transcendentals=0),
        name='layer_grads',
    )(*args)
    return [out[i:i + 2] for i in range(0, len(out), 2)]


def gather(x):
    return lax.all_gather(x, 'data', axis=0)


def local_step(q_loc, d_loc, temperature, q_w1, q_w2, q_proj, d_w1, d_w2, d_proj):
    rows, width = q_loc.shape
    me = lax.axis_index('data')
    d_own = d_loc.reshape(2 * rows, width)
    h1_own, d_last, q_last = forward(d_own, q_loc, d_w1, d_w2, q_w1, q_w2)
    d_last = d_last.reshape(-1, width)
    q_last = q_last.reshape(-1, width)
    h1_all = gather(h1_own)
    d_own, q_own, _ = lax.optimization_barrier((d_own, q_loc, h1_own))
    h0_all = gather(jnp.concatenate([d_own, q_own], axis=0))
    docs = dot(d_last, d_proj).astype(BF16)
    queries = dot(q_last, q_proj).astype(BF16)
    batch = queries.shape[0]
    logits = dot_nt(queries, docs) / temperature
    row = jnp.arange(batch)
    target = jnp.arange(2 * batch)[None, :] == ((row // rows) * 2 * rows + row % rows)[:, None]
    log_norm = jax.nn.logsumexp(logits, axis=1)
    pos = jnp.sum(jnp.where(target, logits, 0.0), axis=1)
    loss = jnp.sum(log_norm - pos) / batch
    prob = jnp.exp(logits - log_norm[:, None])
    grad = ((prob - target.astype(F32)) / (batch * temperature)).astype(BF16)
    q_up = dot(grad, docs).astype(BF16)
    d_up = dot_tn(grad, queries).astype(BF16)

    def start(up, proj):
        own = up.shape[0] // 16
        return dot_nt(lax.dynamic_slice_in_dim(up, me * own, own, 0), proj)

    e0_all = gather(chain(h1_own, start(d_up, d_proj), start(q_up, q_proj), d_w1, d_w2, q_w1, q_w2))
    d_up, d_last = [x.reshape(16, 2 * rows, width) for x in (d_up, d_last)]
    q_up, q_last = [x.reshape(16, rows, width) for x in (q_up, q_last)]
    core = (me % 2).reshape(1)

    def swap(halves):
        return [lax.ppermute(x, 'data', [(i, i ^ 1) for i in range(16)]) for x in halves]

    q_g, q1, (q_p,) = layer_grads(core, 1, None, h1_all, 2, q_up, 0, rows, q_w1, q_w2, top=(q_proj, q_last))
    q1 = swap(q1)
    d_g, d1, (d_p,) = layer_grads(core, 1, None, h1_all, 0, d_up, 0, 2 * rows, d_w1, d_w2, top=(d_proj, d_last))
    d1 = swap(d1)
    d_g, d0, q_g = layer_grads(core, 0, None, h0_all, 0, e0_all, 0, 2 * rows, d_w1, d_w2, d_g, (1, q1, q_g))
    d0 = swap(d0)
    q_g, d_g = layer_grads(core, 0, 0, h0_all, 2, e0_all, 2, rows, q_w1, q_w2, q_g, (1, d1, d_g))
    q_g, d_g = layer_grads(core, 0, 4, h0_all, 2, e0_all, 2, rows, q_w1, q_w2, q_g, (0, d0, d_g))
    return (loss, *q_g, q_p, *d_g, d_p)


def solution(mesh):
    specs_in = (P('data', None), P(None, 'data', None), P(), P(), P(), P(), P(), P(), P())
    specs_out = (P(), P(), P(), P(), P(), P(), P())
    return jax.shard_map(local_step, mesh=mesh, in_specs=specs_in, out_specs=specs_out, check_vma=False)
```

```python
import functools

import jax
import jax.numpy as jnp
from jax import lax
from jax.experimental import pallas as pl
from jax.experimental.pallas import tpu as pltpu
from jax.sharding import PartitionSpec as P

ROWS_CONTRACT = (((0,), (0,)), ((), ()))
LAST_CONTRACT = (((1,), (1,)), ((), ()))
F32 = jnp.float32
BF16 = jnp.bfloat16
GELU_C = 0.7978845608028654
GELU_D = 0.044715
MIB = 1024 * 1024


def dot(a, b):
    return jnp.dot(a, b, preferred_element_type=F32)


def dot_nt(a, b):
    return lax.dot_general(a, b, LAST_CONTRACT, preferred_element_type=F32)


def dot_tn(a, b):
    return lax.dot_general(a, b, ROWS_CONTRACT, preferred_element_type=F32)


def gelu_cdf(a):
    sq = a * a
    return sq, 0.5 + 0.5 * jnp.tanh(a * (GELU_C + (GELU_C * GELU_D) * sq))


def gelu_and_back(a, t):
    sq, cdf = gelu_cdf(a)
    u = a * cdf
    slope = cdf + u * (1.0 - cdf) * (2.0 * GELU_C + (6.0 * GELU_C * GELU_D) * sq)
    return u.astype(BF16), (slope * t).astype(BF16)


BLOCK = 1024
RING = 4
THIRDS = ((0, 384), (384, 384), (768, 256))
ORDERS = ((2, 4, 8), (4, 8, 2), (8, 2, 4))


def flip(device, bit):
    return device + bit * (1 - 2 * (lax.div(device, bit) % 2))


def forward_kernel(xd_ref, xq_ref, dw1_ref, dw2_ref, qw1_ref, qw2_ref, h1_ref, d_all, q_all, acc_ref, h_ref, h2_ref,
                   w1_buf, w2_buf, w1_sem, w2_sem, send_sem, recv_sem, pair_send, pair_recv, own_sem, own_send, own_recv):
    s = pl.program_id(0)
    per = dw1_ref.shape[2] // BLOCK
    slot = s % RING
    me = lax.axis_index('data')
    partner = flip(me, 1)
    d_rows = d_all.shape[1]
    q_rows = q_all.shape[1]
    towers = ((pl.ds(0, d_rows), d_all), (pl.ds(d_rows, q_rows), q_all))

    def walk(p, mask):
        device = me
        for i in range(3):
            if mask & (1 << i):
                device = flip(device, ORDERS[p][i])
        return device

    def remote(source, target, send, recv, device):
        return pltpu.make_async_remote_copy(src_ref=source, dst_ref=target, send_sem=send, recv_sem=recv,
                                            device_id=(device,), device_id_type=pl.DeviceIdType.MESH)

    def hop(t, p, mask, step):
        rows, out = towers[t]
        cols = pl.ds(*THIRDS[p])
        shard = walk(p, mask)
        source = h2_ref.at[rows, cols] if mask == 0 else out.at[shard, :, cols]
        seen = mask | (1 << step)
        return remote(source, out.at[shard, :, cols], send_sem.at[t, p, seen], recv_sem.at[t, p, seen], flip(me, ORDERS[p][step]))

    def relay(t, p, mask):
        part = towers[t][1].at[walk(p, mask), :, pl.ds(*THIRDS[p])]
        return remote(part, part, pair_send.at[t, p, mask], pair_recv.at[t, p, mask], partner)

    def arrived(t, p, mask):
        part = towers[t][1].at[walk(p, mask), :, pl.ds(*THIRDS[p])]
        remote(part, part, send_sem.at[t, p, mask], recv_sem.at[t, p, mask], partner).wait_recv()

    def own_pair(t):
        rows, out = towers[t]
        return remote(h2_ref.at[rows], out.at[me], own_send.at[t], own_recv.at[t], partner)

    def own_copy(t):
        rows, out = towers[t]
        return pltpu.make_async_copy(h2_ref.at[rows], out.at[me], own_sem.at[t])

    def begin(t):
        for step in range(3):
            for p in range(3):
                hop(t, p, 0, step).start()
        own_copy(t).start()
        own_pair(t).start()

    def onward(t, masks):
        for mask in masks:
            for p in range(3):
                arrived(t, p, mask)
                for step in range(mask.bit_length(), 3):
                    hop(t, p, mask, step).start()
                relay(t, p, mask).start()

    def blocks(step, w1_ref, w2_ref):
        layer = (step // per) % 2
        cols = pl.ds((step % per) * BLOCK, BLOCK)
        at = step % RING
        return (pltpu.make_async_copy(w1_ref.at[layer, :, cols], w1_buf.at[at], w1_sem.at[at]),
                pltpu.make_async_copy(w2_ref.at[layer, cols, :], w2_buf.at[at], w2_sem.at[at]))

    def fetch(step):
        @pl.when(step < 2 * per)
        def _():
            for copy in blocks(step, dw1_ref, dw2_ref):
                copy.start()

        @pl.when((step >= 2 * per) & (step < 4 * per))
        def _():
            for copy in blocks(step, qw1_ref, qw2_ref):
                copy.start()

    def layers(first, rows, x_ref, w1_ref, w2_ref):
        for copy in blocks(s, w1_ref, w2_ref):
            copy.wait()

        @pl.when(s == first)
        def _():
            h_ref[rows, :] = x_ref[...]

        @pl.when((s - first) % per == 0)
        def _():
            acc_ref[rows, :] = h_ref[rows, :].astype(F32)

        pre = dot(h_ref[rows, :], w1_buf[slot])
        acc_ref[rows, :] += dot((pre * gelu_cdf(pre)[1]).astype(BF16), w2_buf[slot])

        @pl.when(s == first + per - 1)
        def _():
            h1 = acc_ref[rows, :].astype(BF16)
            h_ref[rows, :] = h1
            h1_ref[rows, :] = h1

        @pl.when(s == first + 2 * per - 1)
        def _():
            h2_ref[rows, :] = acc_ref[rows, :].astype(BF16)

    @pl.when(s == 0)
    def _():
        for step in range(RING - 1):
            for copy in blocks(step, dw1_ref, dw2_ref):
                copy.start()
        barrier = pltpu.get_barrier_semaphore()
        for bit in (1, 2, 4, 8):
            pl.semaphore_signal(barrier, inc=1, device_id=(flip(me, bit),), device_id_type=pl.DeviceIdType.MESH)
        pl.semaphore_wait(barrier, 4)

    fetch(s + RING - 1)

    @pl.when(s == 2 * per)
    def _():
        begin(0)

    @pl.when(s == 2 * per + per // 2)
    def _():
        onward(0, (1,))

    @pl.when(s == 3 * per)
    def _():
        onward(0, (2,))

    @pl.when(s == 3 * per + per // 4)
    def _():
        onward(0, (3,))

    @pl.when(s < 2 * per)
    def _():
        layers(0, towers[0][0], xd_ref, dw1_ref, dw2_ref)

    @pl.when((s >= 2 * per) & (s < 4 * per))
    def _():
        layers(2 * per, towers[1][0], xq_ref, qw1_ref, qw2_ref)

    @pl.when(s == 4 * per)
    def _():
        begin(1)
        onward(0, (4, 5, 6, 7))
        onward(1, (1, 2, 3, 4, 5, 6, 7))
        for t in range(2):
            for p in range(3):
                for mask in range(8):
                    for step in range(mask.bit_length(), 3):
                        hop(t, p, mask, step).wait_send()
                    if mask:
                        relay(t, p, mask).wait()
            own_copy(t).wait()
            own_pair(t).wait()


def forward(d_own, q_own, d_w1, d_w2, q_w1, q_w2):
    third, width = q_own.shape
    rows = 3 * third
    per = d_w1.shape[2] // BLOCK

    anywhere = pl.BlockSpec(memory_space=pl.ANY)
    sems = pltpu.SemaphoreType.DMA
    return pl.pallas_call(
        forward_kernel,
        grid=(4 * per + 1,),
        in_specs=[pl.BlockSpec((2 * third, width), lambda s: (0, 0)), pl.BlockSpec((third, width), lambda s: (0, 0)),
                  *[anywhere] * 4],
        out_specs=[pl.BlockSpec((rows, width), lambda s: (0, 0))] + [anywhere] * 2,
        out_shape=[jax.ShapeDtypeStruct((rows, width), BF16), jax.ShapeDtypeStruct((16, 2 * third, width), BF16),
                   jax.ShapeDtypeStruct((16, third, width), BF16)],
        scratch_shapes=[pltpu.VMEM((rows, width), F32), pltpu.VMEM((rows, width), BF16), pltpu.VMEM((rows, width), BF16),
                        pltpu.VMEM((RING, width, BLOCK), BF16), pltpu.VMEM((RING, BLOCK, width), BF16), sems((RING,)), sems((RING,)),
                        sems((2, 3, 8)), sems((2, 3, 8)), sems((2, 3, 8)), sems((2, 3, 8)), sems((2,)), sems((2,)), sems((2,))],
        compiler_params=pltpu.CompilerParams(collective_id=0, has_side_effects=True, dimension_semantics=('arbitrary',)),
        cost_estimate=pl.CostEstimate(flops=8 * rows * width * d_w1.shape[2], bytes_accessed=72 * MIB, transcendentals=0),
        name='forward',
    )(d_own, q_own, d_w1, d_w2, q_w1, q_w2)


def chain_kernel(me_ref, h_ref, d_up, q_up, d_proj, q_proj, dw1_ref, dw2_ref, qw1_ref, qw2_ref, out_ref, acc_ref, e_ref):
    s = pl.program_id(0)
    third = h_ref.shape[0] // 3
    parts = ((pl.ds(0, 2 * third), dw1_ref, dw2_ref), (pl.ds(2 * third, third), qw1_ref, qw2_ref))

    @pl.when(s == 0)
    def _():
        for (rows, _, _), up_ref, proj_ref in zip(parts, (d_up, q_up), (d_proj, q_proj)):
            e1 = dot_nt(up_ref[0], proj_ref[...])
            acc_ref[rows, :] = e1
            e_ref[rows, :] = e1.astype(BF16)

    pre = [dot(h_ref[rows, :], w1_ref[0]) for rows, w1_ref, _ in parts]
    t = [dot_nt(e_ref[rows, :], w2_ref[0]) for rows, _, w2_ref in parts]
    delta = [gelu_and_back(*pair)[1] for pair in zip(pre, t)]
    for (rows, w1_ref, _), d in zip(parts, delta):
        acc_ref[rows, :] += dot_nt(d, w1_ref[0])

    @pl.when(s == pl.num_programs(0) - 1)
    def _():
        out_ref[...] = acc_ref[...].astype(BF16)


def chain(me, h1_own, d_up, q_up, d_proj, q_proj, d_w1, d_w2, q_w1, q_w2):
    rows, width = h1_own.shape
    block = 512
    wide = pl.BlockSpec((1, width, block), lambda s, m: (1, 0, s))
    tall = pl.BlockSpec((1, block, width), lambda s, m: (1, s, 0))

    def whole(x):
        return pl.BlockSpec(x.shape, lambda s, m: (0, 0))

    def own(x):
        return pl.BlockSpec((1, *x.shape[1:]), lambda s, m: (m[0], 0, 0))

    return pl.pallas_call(
        chain_kernel,
        grid_spec=pltpu.PrefetchScalarGridSpec(
            num_scalar_prefetch=1, grid=(d_w1.shape[2] // block,),
            in_specs=[whole(h1_own), own(d_up), own(q_up), whole(d_proj), whole(q_proj), wide, tall, wide, tall],
            out_specs=whole(h1_own),
            scratch_shapes=[pltpu.VMEM((rows, width), F32), pltpu.VMEM((rows, width), BF16)]),
        out_shape=jax.ShapeDtypeStruct((rows, width), BF16),
        compiler_params=pltpu.CompilerParams(dimension_semantics=('arbitrary',)),
        cost_estimate=pl.CostEstimate(flops=4 * rows * width * d_w1.shape[2], bytes_accessed=40 * MIB, transcendentals=0),
        name='chain',
    )(me.reshape(1), h1_own, d_up, q_up, d_proj, q_proj, d_w1, d_w2, q_w1, q_w2)


def layer_kernel(row_tile, in_place, incoming, send, top, core_ref, h_ref, e_ref, w1_ref, w2_ref, *rest):
    if top:
        up_ref, (proj_ref, last_ref), e_ref, rest = e_ref, rest[:2], rest[-1], rest[2:-1]
    u_ref, delta_ref = rest[-2:]
    rest = rest[2 if in_place else 0:-2]
    if incoming:
        y_refs, rest = rest[:2], rest[4:]
        for y_ref, t_ref in zip(y_refs, rest[-2:]):
            t_ref[...] = y_ref[...]
        rest = rest[:-2]
    one_ref, two_ref = rest[:2]
    n, r, width = h_ref.shape
    h = h_ref.reshape(n * r, width)
    e = e_ref.reshape(n * r, width)
    if top:
        up = up_ref.reshape(n * r, width)

        @pl.when(pl.program_id(0) == 0)
        def _():
            for i in range(n * r // row_tile):
                rows = pl.ds(i * row_tile, row_tile)
                e_ref[rows, :] = dot_nt(up[rows, :], proj_ref[...]).astype(BF16)

        rest[4][...] = dot_tn(last_ref.reshape(n * r, last_ref.shape[2])[...], up[...])
    w1_t = w1_ref[0].T
    for i in range(n * r // row_tile):
        rows = pl.ds(i * row_tile, row_tile)
        pre = dot_nt(w1_t, h[rows, :])
        t = dot_nt(w2_ref[0], e[rows, :])
        u_ref[:, rows], delta_ref[:, rows] = gelu_and_back(pre, t)
    for c in range(4):
        cols = pl.ds(c * (width // 4), width // 4)
        two = dot(u_ref[...], e[:, cols])
        one = dot(delta_ref[...], h[:, cols]).T
        two_ref[0, :, cols] = two
        one_ref[0, cols, :] = one
        if send:
            rest[3][0, :, cols] = two
            rest[2][0, cols, :] = one


def layer_grads(core, layer, first, h_all, h_place, e_all, e_place, rows, w1, w2, grads=None, incoming=None, top=None):
    _, width, ffn_width = w1.shape
    n = h_all.shape[0]
    block, row_tile, steps = 512, 512, 4
    total = n * rows
    send = first is None
    resident = pl.Buffered(buffer_count=1)

    def mine(j, c):
        return c[0] * steps + j if send else first + j

    def other(j, c):
        return (1 - c[0]) * steps + j

    def wide(at, place):
        return pl.BlockSpec((1, width, block), lambda j, c: (at, 0, place(j, c)))

    def tall(at, place):
        return pl.BlockSpec((1, block, width), lambda j, c: (at, place(j, c), 0))

    in_specs = [
        pl.BlockSpec((n, rows, width), lambda j, c: (0, h_place, 0), pipeline_mode=resident),
        pl.BlockSpec((n, rows, width), lambda j, c: (0, e_place, 0), pipeline_mode=resident),
        wide(layer, mine), tall(layer, mine),
    ]
    args = [core, h_all, e_all, w1, w2]
    out_specs = [wide(layer, mine), tall(layer, mine)]
    out_shape = [jax.ShapeDtypeStruct(w1.shape, F32), jax.ShapeDtypeStruct(w2.shape, F32)]
    aliases = {}
    anywhere = [pl.BlockSpec(memory_space=pl.ANY)] * 2
    scratch = [pltpu.VMEM((block, total), BF16)] * 2
    if top is not None:
        in_specs += [pl.BlockSpec((width, width), lambda j, c: (0, 0), pipeline_mode=resident),
                     pl.BlockSpec((n, rows, width // steps), lambda j, c: (0, 0, j))]
        args += list(top)
        scratch.append(pltpu.VMEM((total, width), BF16))
    if grads is not None:
        aliases.update({len(args): 0, len(args) + 1: 1})
        in_specs += anywhere
        args += list(grads)
    if send:
        out_specs += [wide(0, lambda j, c: j), tall(0, lambda j, c: j)]
        out_shape += [jax.ShapeDtypeStruct((1, width, ffn_width // 2), F32), jax.ShapeDtypeStruct((1, ffn_width // 2, width), F32)]
    if top is not None:
        out_specs.append(pl.BlockSpec((width // steps, width), lambda j, c: (j, 0)))
        out_shape.append(jax.ShapeDtypeStruct((width, width), F32))
    if incoming is not None:
        at, halves, targets = incoming
        in_specs += [wide(0, lambda j, c: j), tall(0, lambda j, c: j)] + anywhere
        aliases.update({len(args) + 2: len(out_shape), len(args) + 3: len(out_shape) + 1})
        args += [*halves, *targets]
        out_specs += [wide(at, other), tall(at, other)]
        out_shape += [jax.ShapeDtypeStruct(t.shape, F32) for t in targets]
    out = pl.pallas_call(
        functools.partial(layer_kernel, row_tile, grads is not None, incoming is not None, send, top is not None),
        grid_spec=pltpu.PrefetchScalarGridSpec(
            num_scalar_prefetch=1, grid=(steps,), in_specs=in_specs, out_specs=out_specs,
            scratch_shapes=scratch),
        out_shape=out_shape,
        input_output_aliases=aliases,
        compiler_params=pltpu.CompilerParams(vmem_limit_bytes=58 * MIB, dimension_semantics=('arbitrary',)),
        cost_estimate=pl.CostEstimate(flops=8 * total * width * block * steps, bytes_accessed=40 * MIB, transcendentals=0),
        name='layer_grads',
    )(*args)
    return [out[i:i + 2] for i in range(0, len(out), 2)]


def gather(x):
    return lax.all_gather(x, 'data', axis=0)


def local_step(q_loc, d_loc, temperature, q_w1, q_w2, q_proj, d_w1, d_w2, d_proj):
    rows, width = q_loc.shape
    me = lax.axis_index('data')
    d_own = d_loc.reshape(2 * rows, width)
    h1_own, d_last, q_last = forward(d_own, q_loc, d_w1, d_w2, q_w1, q_w2)
    d_last = d_last.reshape(-1, width)
    q_last = q_last.reshape(-1, width)
    h1_all = gather(h1_own)
    d_own, q_own, _ = lax.optimization_barrier((d_own, q_loc, h1_own))
    h0_all = gather(jnp.concatenate([d_own, q_own], axis=0))
    docs = dot(d_last, d_proj).astype(BF16)
    queries = dot(q_last, q_proj).astype(BF16)
    batch = queries.shape[0]
    logits = dot_nt(queries, docs) / temperature
    row = jnp.arange(batch)
    target = jnp.arange(2 * batch)[None, :] == ((row // rows) * 2 * rows + row % rows)[:, None]
    log_norm = jax.nn.logsumexp(logits, axis=1)
    pos = jnp.sum(jnp.where(target, logits, 0.0), axis=1)
    loss = jnp.sum(log_norm - pos) / batch
    prob = jnp.exp(logits - log_norm[:, None])
    grad = ((prob - target.astype(F32)) / (batch * temperature)).astype(BF16)
    q_up = dot(grad, docs).astype(BF16)
    d_up = dot_tn(grad, queries).astype(BF16)

    d_up, d_last = [x.reshape(16, 2 * rows, width) for x in (d_up, d_last)]
    q_up, q_last = [x.reshape(16, rows, width) for x in (q_up, q_last)]
    e0_all = gather(chain(me, h1_own, d_up, q_up, d_proj, q_proj, d_w1, d_w2, q_w1, q_w2))
    core = (me % 2).reshape(1)

    def swap(halves):
        return [lax.ppermute(x, 'data', [(i, i ^ 1) for i in range(16)]) for x in halves]

    q_g, q1, (q_p,) = layer_grads(core, 1, None, h1_all, 2, q_up, 0, rows, q_w1, q_w2, top=(q_proj, q_last))
    q1 = swap(q1)
    d_g, d1, (d_p,) = layer_grads(core, 1, None, h1_all, 0, d_up, 0, 2 * rows, d_w1, d_w2, top=(d_proj, d_last))
    d1 = swap(d1)
    d_g, d0, q_g = layer_grads(core, 0, None, h0_all, 0, e0_all, 0, 2 * rows, d_w1, d_w2, d_g, (1, q1, q_g))
    d0 = swap(d0)
    q_g, d_g = layer_grads(core, 0, 0, h0_all, 2, e0_all, 2, rows, q_w1, q_w2, q_g, (1, d1, d_g))
    q_g, d_g = layer_grads(core, 0, 4, h0_all, 2, e0_all, 2, rows, q_w1, q_w2, q_g, (0, d0, d_g))
    return (loss, *q_g, q_p, *d_g, d_p)


def solution(mesh):
    specs_in = (P('data', None), P(None, 'data', None), P(), P(), P(), P(), P(), P(), P())
    specs_out = (P(), P(), P(), P(), P(), P(), P())
    return jax.shard_map(local_step, mesh=mesh, in_specs=specs_in, out_specs=specs_out, check_vma=False)
```
